32 devices in a mesh: dp: 2 (over x), tp: 4 (over z), pp: 4 (over y, core).
Axes of the slice: x: 2, y: 2, z: 4, core: 2. Of those that a mesh axis runs over, the one named last changes fastest.
Arguments:
- hidden: bfloat16 [4, 64, 2048], P('dp'), parts along dimension 0
- positions: int32 [4, 64], P('dp'), parts along dimension 0
- key_cache: bfloat16 [4, 4, 64, 4, 512, 64], P('pp', 'dp', None, 'tp'), parts along dimension 1
- value_cache: bfloat16 [4, 4, 64, 4, 512, 64], P('pp', 'dp', None, 'tp'), parts along dimension 1
- attn_norm: bfloat16 [4, 2048], P('pp')
- w_query: bfloat16 [4, 2048, 2048], P('pp', None, 'tp')
- w_key: bfloat16 [4, 2048, 256], P('pp', None, 'tp')
- w_value: bfloat16 [4, 2048, 256], P('pp', None, 'tp')
- w_out: bfloat16 [4, 2048, 2048], P('pp', 'tp')
- mlp_norm: bfloat16 [4, 2048], P('pp')
- w_gate: bfloat16 [4, 2048, 5632], P('pp', None, 'tp')
- w_up: bfloat16 [4, 2048, 5632], P('pp', None, 'tp')
- w_down: bfloat16 [4, 5632, 2048], P('pp', 'tp')
Outputs:
- output 1: bfloat16 [4, 64, 2048], P('dp'), parts along dimension 0
- output 2: bfloat16 [4, 4, 64, 4, 512, 64], P('pp', 'dp', None, 'tp'), parts along dimension 1
- output 3: bfloat16 [4, 4, 64, 4, 512, 64], P('pp', 'dp', None, 'tp'), parts along dimension 1
There are 2 independent parts. The reference program is written for one: setup_inputs(seed, part) draws one part's arguments, and reference() takes and returns one part's arrays. A program takes and returns all parts, laid end to end along the dimension named above; an argument that names none is the same for every part.
All inputs are finite; a program needn't handle non-finite values.
Results may differ from the reference program's by a relative error of at most 0.02.
Values are sent between devices in bfloat16 or wider.
A program may use at most 1 GiB of HBM per device.

```python
import math
import jax
import jax.numpy as jnp
from jax import lax

D = 2048
HEADS = 32
KV_HEADS = 4
HEAD = 64
FF = 5632
GROUPS = 2
BATCH = 64
SEQ = 512
LAYERS = 4

ROPE_THETA = 500000.0
SCALE_FACTOR = 8.0
LOW_FACTOR = 1.0
HIGH_FACTOR = 4.0
ORIG_CONTEXT = 8192.0
NORM_EPS = 1e-5
GQA_SIZE = HEADS // KV_HEADS


def rope_freqs():
    freq_index = jnp.arange(HEAD // 2, dtype=jnp.float32)
    base_freq = ROPE_THETA ** (-2.0 * freq_index / HEAD)
    wave_len = 2.0 * math.pi / base_freq
    smooth_t = (ORIG_CONTEXT / wave_len - LOW_FACTOR) / (HIGH_FACTOR - LOW_FACTOR)
    mixed_freq = (1.0 - smooth_t) * base_freq / SCALE_FACTOR + smooth_t * base_freq
    long_freq = jnp.where(wave_len > ORIG_CONTEXT / LOW_FACTOR, base_freq / SCALE_FACTOR, mixed_freq)
    return jnp.where(wave_len < ORIG_CONTEXT / HIGH_FACTOR, base_freq, long_freq)


def rms_norm(values, gain_vec):
    values_f = values.astype(jnp.float32)
    inv_rms = lax.rsqrt(jnp.mean(values_f * values_f, axis=-1, keepdims=True) + NORM_EPS)
    return (values_f * inv_rms * gain_vec.astype(jnp.float32)).astype(jnp.bfloat16)


def rotate(values_f, cosine, sine_t):
    half_dim = values_f.shape[-1] // 2
    first_half = values_f[..., :half_dim]
    second_half = values_f[..., half_dim:]
    return jnp.concatenate([first_half * cosine - second_half * sine_t, second_half * cosine + first_half * sine_t], axis=-1)


def setup_inputs(seed: int = 0, part: int = 0) -> dict:
    root_key = jax.random.key(seed)
    part_keys = jax.random.split(jax.random.fold_in(root_key, part), 5)
    weight_keys = jax.random.split(root_key, 9)
    hidden = jax.random.normal(part_keys[0], (GROUPS, BATCH, D), jnp.float32)
    group_len = jax.random.randint(part_keys[1], (GROUPS,), max(SEQ // 8, 1), SEQ + 1, dtype=jnp.int32)
    raw_pos = jax.random.randint(part_keys[2], (GROUPS, BATCH), 0, SEQ, dtype=jnp.int32)
    positions = ((raw_pos * group_len[:, None]) // SEQ).at[0, 0].set(SEQ - 1)
    cache_shape = (LAYERS, GROUPS, BATCH, KV_HEADS, SEQ, HEAD)
    key_cache = jax.random.normal(part_keys[3], cache_shape, jnp.float32)
    value_cache = jax.random.normal(part_keys[4], cache_shape, jnp.float32)
    attn_norm = 1.0 + 0.3 * jax.random.normal(weight_keys[0], (LAYERS, D), jnp.float32)
    w_query = jax.random.normal(weight_keys[1], (LAYERS, D, HEADS * HEAD), jnp.float32) * D ** -0.5
    w_key = jax.random.normal(weight_keys[2], (LAYERS, D, KV_HEADS * HEAD), jnp.float32) * D ** -0.5
    w_value = jax.random.normal(weight_keys[3], (LAYERS, D, KV_HEADS * HEAD), jnp.float32) * D ** -0.5
    w_out = jax.random.normal(weight_keys[4], (LAYERS, HEADS * HEAD, D), jnp.float32) * 2.0 * (HEADS * HEAD) ** -0.5
    mlp_norm = jax.random.normal(weight_keys[5], (LAYERS, D), jnp.float32)
    w_gate = jax.random.normal(weight_keys[6], (LAYERS, D, FF), jnp.float32) * D ** -0.5
    w_up = jax.random.normal(weight_keys[7], (LAYERS, D, FF), jnp.float32) * D ** -0.5
    w_down = jax.random.normal(weight_keys[8], (LAYERS, FF, D), jnp.float32) * FF ** -0.5
    return {
        "hidden": hidden.astype(jnp.bfloat16),
        "positions": positions,
        "key_cache": key_cache.astype(jnp.bfloat16),
        "value_cache": value_cache.astype(jnp.bfloat16),
        "attn_norm": attn_norm.astype(jnp.bfloat16),
        "w_query": w_query.astype(jnp.bfloat16),
        "w_key": w_key.astype(jnp.bfloat16),
        "w_value": w_value.astype(jnp.bfloat16),
        "w_out": w_out.astype(jnp.bfloat16),
        "mlp_norm": mlp_norm.astype(jnp.bfloat16),
        "w_gate": w_gate.astype(jnp.bfloat16),
        "w_up": w_up.astype(jnp.bfloat16),
        "w_down": w_down.astype(jnp.bfloat16),
    }


def reference(hidden, positions, key_cache, value_cache, attn_norm, w_query, w_key, w_value, w_out, mlp_norm, w_gate, w_up, w_down):
    inv_freq = rope_freqs()
    seq_rows = jnp.arange(SEQ)

    def one_layer(state_h, layer_in):
        key_l, value_l, gain_attn, wq_l, wk_l, wv_l, wo_l, gain_mlp, wg_l, wu_l, wd_l = layer_in

        def one_group(group_in):
            tokens, key_g, value_g, pos_g = group_in
            angles = pos_g.astype(jnp.float32)[:, None] * inv_freq
            cosine = jnp.cos(angles)
            sine_t = jnp.sin(angles)
            normed = rms_norm(tokens, gain_attn)
            query_f = jnp.dot(normed, wq_l, preferred_element_type=jnp.float32).reshape(BATCH, KV_HEADS, GQA_SIZE, HEAD)
            query_h = rotate(query_f, cosine[:, None, None, :], sine_t[:, None, None, :]).astype(jnp.bfloat16)
            key_f = jnp.dot(normed, wk_l, preferred_element_type=jnp.float32).reshape(BATCH, KV_HEADS, HEAD)
            key_new = rotate(key_f, cosine[:, None, :], sine_t[:, None, :]).astype(jnp.bfloat16)
            value_new = jnp.dot(normed, wv_l, preferred_element_type=jnp.float32).astype(jnp.bfloat16).reshape(BATCH, KV_HEADS, HEAD)
            row_hit = (seq_rows[None, :] == pos_g[:, None])[:, None, :, None]
            key_g = jnp.where(row_hit, key_new[:, :, None, :], key_g)
            value_g = jnp.where(row_hit, value_new[:, :, None, :], value_g)
            scores = jnp.einsum("bkgd,bksd->bkgs", query_h.astype(jnp.float32), key_g.astype(jnp.float32)) * HEAD ** -0.5
            visible = (seq_rows[None, :] <= pos_g[:, None])[:, None, None, :]
            attn_probs = jax.nn.softmax(jnp.where(visible, scores, -jnp.inf), axis=-1).astype(jnp.bfloat16)
            attn_vals = jnp.einsum("bkgs,bksd->bkgd", attn_probs.astype(jnp.float32), value_g.astype(jnp.float32)).astype(jnp.bfloat16).reshape(BATCH, HEADS * HEAD)
            attn_out = jnp.dot(attn_vals, wo_l, preferred_element_type=jnp.float32).astype(jnp.bfloat16)
            mid_state = (tokens.astype(jnp.float32) + attn_out.astype(jnp.float32)).astype(jnp.bfloat16)
            normed_mlp = rms_norm(mid_state, gain_mlp)
            gate_f = jnp.dot(normed_mlp, wg_l, preferred_element_type=jnp.float32)
            up_f = jnp.dot(normed_mlp, wu_l, preferred_element_type=jnp.float32)
            act_bf = (jax.nn.silu(gate_f) * up_f).astype(jnp.bfloat16)
            mlp_out = jnp.dot(act_bf, wd_l, preferred_element_type=jnp.float32).astype(jnp.bfloat16)
            new_state = (mid_state.astype(jnp.float32) + mlp_out.astype(jnp.float32)).astype(jnp.bfloat16)
            return new_state, key_g, value_g

        new_state, key_l, value_l = lax.map(one_group, (state_h, key_l, value_l, positions))
        return new_state, (key_l, value_l)

    final_state, caches = lax.scan(one_layer, hidden, (key_cache, value_cache, attn_norm, w_query, w_key, w_value, w_out, mlp_norm, w_gate, w_up, w_down))
    return final_state, caches[0], caches[1]
```

```python
import functools
import math
import jax
import jax.numpy as jnp
from jax import lax
from jax.experimental import pallas as pl
from jax.experimental.pallas import tpu as pltpu
from jax.sharding import PartitionSpec as P

ROPE_THETA = 500000.0
SCALE_FACTOR = 8.0
LOW_FACTOR = 1.0
HIGH_FACTOR = 4.0
ORIG_CONTEXT = 8192.0
NORM_EPS = 1e-5

MESH = pl.DeviceIdType.MESH
F32 = jnp.float32
BF16 = jnp.bfloat16

T = 64
NC = 4


def rope_freqs(head_dim):
    freq_index = jnp.arange(head_dim // 2, dtype=F32)
    base_freq = ROPE_THETA ** (-2.0 * freq_index / head_dim)
    wave_len = 2.0 * math.pi / base_freq
    smooth_t = (ORIG_CONTEXT / wave_len - LOW_FACTOR) / (HIGH_FACTOR - LOW_FACTOR)
    mixed_freq = (1.0 - smooth_t) * base_freq / SCALE_FACTOR + smooth_t * base_freq
    long_freq = jnp.where(wave_len > ORIG_CONTEXT / LOW_FACTOR, base_freq / SCALE_FACTOR, mixed_freq)
    return jnp.where(wave_len < ORIG_CONTEXT / HIGH_FACTOR, base_freq, long_freq)


def dot(lhs, rhs):
    return jnp.dot(lhs, rhs, preferred_element_type=F32)


def dot_nt(lhs, rhs):
    return lax.dot_general(lhs, rhs, (((1,), (1,)), ((), ())), preferred_element_type=F32)


def layer_kernel(
    nm, hid_hbm, pos_ref, cos_ref, sin_ref, ga_ref, gm_ref, wq_hbm, wk_hbm, wv_hbm, wo_hbm, wg_hbm, wu_hbm, wd_hbm, kc_hbm, vc_hbm,
    out_ref, kv_ref,
    wq, wkv, wo, wgu, wd, kc, vc, hin, hmid, norm, qs, ks, vs, att, act, part, send_a, recv_a, recv_b, nxt, fin,
    w_sem, kv_sem, h_sem, hin_sem, hmid_sem, a_sem, b_sem, fin_sem, sa_sem, sm_sem, sn_sem, sf_sem,
):
    tp = lax.axis_index("tp")
    pp = lax.axis_index("pp")
    n_tp, n_pp = 4, 4
    last = n_pp - 1
    is_end = (tp == 0) | (tp == n_tp - 1)
    is_mid = jnp.logical_not(is_end)
    side = tp + 1 - 2 * lax.rem(tp, 2)
    across = n_tp - 1 - tp
    d_model = norm.shape[-1]
    width = d_model // NC
    ff = act.shape[-1]

    def hidden_copy(i, c):
        return pltpu.make_async_copy(hid_hbm.at[i, :, pl.ds(c * width, width)], hin.at[i, c], h_sem.at[i, c])

    @pl.when(pp == 0)
    def _():
        for c in range(NC):
            hidden_copy(0, c).start()

    load_q = [pltpu.make_async_copy(wq_hbm, wq, w_sem.at[0])]
    load_kv = [
        pltpu.make_async_copy(wk_hbm, wkv.at[pl.ds(0, 64)], w_sem.at[1]),
        pltpu.make_async_copy(wv_hbm, wkv.at[pl.ds(64, 64)], w_sem.at[2]),
    ]
    load_o = [pltpu.make_async_copy(wo_hbm, wo, w_sem.at[3])]
    load_d = [pltpu.make_async_copy(wd_hbm, wd, w_sem.at[4])]
    load_gu = []
    for j in range(ff // 128):
        load_gu.append(pltpu.make_async_copy(wg_hbm.at[:, pl.ds(128 * j, 128)], wgu.at[:, pl.ds(256 * j, 128)], w_sem.at[5 + 2 * j]))
        load_gu.append(pltpu.make_async_copy(wu_hbm.at[:, pl.ds(128 * j, 128)], wgu.at[:, pl.ds(256 * j + 128, 128)], w_sem.at[6 + 2 * j]))

    def cache_copies(i):
        return [pltpu.make_async_copy(kc_hbm.at[i], kc.at[i], kv_sem.at[0, i]), pltpu.make_async_copy(vc_hbm.at[i], vc.at[i], kv_sem.at[1, i])]

    for copy in load_q + load_kv + cache_copies(0) + load_o + load_gu + load_d:
        copy.start()
    for i in range(1, nm):
        @pl.when(pp == 0)
        def _():
            for c in range(NC):
                hidden_copy(i, c).start()
        for copy in cache_copies(i):
            copy.start()

    barrier = pltpu.get_barrier_semaphore()
    me = tp * n_pp + pp
    for step in range(1, n_tp * n_pp):
        peer = lax.rem(me + step, n_tp * n_pp)
        pl.semaphore_signal(barrier, inc=1, device_id={"tp": peer // n_pp, "pp": lax.rem(peer, n_pp)}, device_id_type=MESH)
    pl.semaphore_wait(barrier, n_tp * n_pp - 1)

    def send(src, dst, s_sem, r_sem, to_tp, to_pp):
        return pltpu.make_async_remote_copy(src_ref=src, dst_ref=dst, send_sem=s_sem, recv_sem=r_sem, device_id={"tp": to_tp, "pp": to_pp}, device_id_type=MESH)

    def end_to_mid(i, k, c):
        return send(send_a.at[i, k, c], recv_a.at[i, k, c], sa_sem.at[i, k, c], a_sem.at[i, k, c], side, pp)

    def mid_to_mid(i, k, c):
        return send(send_a.at[i, k, c], recv_b.at[i, k, c], sa_sem.at[i, k, c], b_sem.at[i, k, c], across, pp)

    def mid_to_end(i, c):
        return send(hmid.at[i, c], hmid.at[i, c], sm_sem.at[i, c], hmid_sem.at[i, c], side, pp)

    def to_next(i, c):
        following = lax.rem(pp + 1, n_pp)
        return [
            send(nxt.at[i, c], hin.at[i, c], sn_sem.at[i, c, 0], hin_sem.at[i, c], tp, following),
            send(nxt.at[i, c], hin.at[i, c], sn_sem.at[i, c, 1], hin_sem.at[i, c], side, following),
        ]

    def fin_copy(i, c, slot, to_tp, to_pp):
        return send(fin.at[i, c], fin.at[i, c], sf_sem.at[i, c, slot], fin_sem.at[i, c], to_tp, to_pp)

    lane = lax.broadcasted_iota(jnp.int32, (8, 128), 1)
    row = lax.broadcasted_iota(jnp.int32, (8, 128), 0)
    upper = lane >= 64
    owner = [row == 2 * c + jnp.where(upper, 1, 0) for c in range(4)]
    lane_t = lax.broadcasted_iota(jnp.int32, (T, 128), 1)
    first_half = lax.rem(lane_t, 64) < 32
    lower_t = lane_t < 64
    lane_s = lax.broadcasted_iota(jnp.int32, (8, kc.shape[-1]), 1)

    def rms(src, i, gain_ref):
        total = jnp.zeros((T, 1), F32)
        for c in range(NC):
            x = src[i, c].astype(F32)
            total = total + jnp.sum(x * x, axis=-1, keepdims=True)
        inv = lax.rsqrt(total / d_model + NORM_EPS)
        for c in range(NC):
            cols = pl.ds(c * width, width)
            norm[:, cols] = (src[i, c].astype(F32) * inv * gain_ref[:, cols].astype(F32)).astype(BF16)

    def rotate(x, i):
        swapped = jnp.where(first_half, pltpu.roll(x, 96, 1), pltpu.roll(x, 32, 1))
        return x * cos_ref[i] + swapped * sin_ref[i]

    def attention_block(i, j):
        rows = pl.ds(pl.multiple_of(8 * j, 8), 8)
        cache_rows = pl.ds(pl.multiple_of(512 * j, 512), 512)
        kb = ks[rows, :]
        vb = vs[rows, :]
        seen = lane_s < pos_ref[i, rows, 0:1]
        lhs, fresh = [], []
        for h in range(8):
            x = qs[rows, pl.ds(128 * (h // 2), 128)]
            turned = pltpu.roll(x, 64, 1)
            both = jnp.where(upper, turned, x) if h % 2 == 0 else jnp.where(upper, x, turned)
            lhs.append(jnp.concatenate([jnp.where(o, both, 0.0) for o in owner], axis=1))
            fresh.append(jnp.sum(both * kb, axis=-1, keepdims=True) * 0.5)
        scores = dot(jnp.concatenate(lhs, axis=0).astype(BF16), kc[i, cache_rows, :])
        probs, new_probs = [], []
        for h in range(8):
            s = jnp.where(seen, scores[8 * h:8 * h + 8], -jnp.inf)
            top = jnp.maximum(jnp.max(s, axis=-1, keepdims=True), fresh[h])
            e = jnp.exp((s - top) * 0.125)
            e_new = jnp.exp((fresh[h] - top) * 0.125)
            scale = 1.0 / (jnp.sum(e, axis=-1, keepdims=True) + e_new)
            probs.append(e * scale)
            new_probs.append((e_new * scale).astype(BF16).astype(F32))
        mixed = dot_nt(jnp.concatenate(probs, axis=0).astype(BF16), vc[i, cache_rows, :])
        heads = []
        for h in range(8):
            o = mixed[8 * h:8 * h + 8]
            acc = jnp.where(owner[0], o[:, 0:128], 0.0)
            for c in range(1, 4):
                acc = acc + jnp.where(owner[c], o[:, 128 * c:128 * c + 128], 0.0)
            heads.append(acc + pltpu.roll(acc, 64, 1) + new_probs[h] * vb)
        for p in range(4):
            att[rows, pl.ds(128 * p, 128)] = jnp.where(upper, heads[2 * p + 1], heads[2 * p])

    def give_part(i, k, c, value):
        @pl.when(is_end)
        def _():
            send_a[i, k, c] = value.astype(BF16)
            end_to_mid(i, k, c).start()

        @pl.when(is_mid)
        def _():
            part[i, c] = value

    def attention(i, first):
        @pl.when(pp == 0)
        def _():
            for c in range(NC):
                hidden_copy(i, c).wait()

        @pl.when(pp > 0)
        def _():
            for c in range(NC):
                to_next(i, c)[0].wait_recv()

        rms(hin, i, ga_ref)

        @pl.when(first)
        def _():
            for copy in load_q + load_kv:
                copy.wait()

        n = norm[...]
        q = dot(n, wq[...])
        for p in range(4):
            qs[:, pl.ds(128 * p, 128)] = rotate(q[:, 128 * p:128 * p + 128], i).astype(BF16).astype(F32)
        kv = dot_nt(n, wkv[...])
        kv = jnp.where(lower_t, rotate(kv, i), kv).astype(BF16)
        kv_ref[i] = kv
        kv = kv.astype(F32)
        turned = pltpu.roll(kv, 64, 1)
        ks[...] = jnp.where(lower_t, kv, turned)
        vs[...] = jnp.where(lower_t, turned, kv)
        for copy in cache_copies(i):
            copy.wait()

        @pl.loop(0, T // 8)
        def _(j):
            attention_block(i, j)

        @pl.when(first)
        def _():
            for copy in load_o:
                copy.wait()

        a = att[...].astype(BF16)
        for c in range(NC):
            give_part(i, 0, c, dot(a, wo[:, pl.ds(c * width, width)]))

    def mid_sum(i, k):
        @pl.when(is_mid)
        def _():
            for c in range(NC):
                end_to_mid(i, k, c).wait_recv()
                send_a[i, k, c] = (part[i, c] + recv_a[i, k, c].astype(F32)).astype(BF16)
                mid_to_mid(i, k, c).start()

    def total_of(i, k, c):
        mid_to_mid(i, k, c).wait_recv()
        return (send_a[i, k, c].astype(F32) + recv_b[i, k, c].astype(F32)).astype(BF16).astype(F32)

    def attention_sum(i):
        @pl.when(is_mid)
        def _():
            for c in range(NC):
                hmid[i, c] = (hin[i, c].astype(F32) + total_of(i, 0, c)).astype(BF16)
                mid_to_end(i, c).start()

        @pl.when(is_end)
        def _():
            for c in range(NC):
                mid_to_end(i, c).wait_recv()

    def mlp(i, first):
        rms(hmid, i, gm_ref)

        @pl.when(first)
        def _():
            for copy in load_gu:
                copy.wait()

        n = norm[...]
        for j in range(ff // 128):
            both = dot(n, wgu[:, pl.ds(256 * j, 256)])
            gate = both[:, :128]
            act[:, pl.ds(128 * j, 128)] = (gate * jax.nn.sigmoid(gate) * both[:, 128:]).astype(BF16)

        @pl.when(first)
        def _():
            for copy in load_d:
                copy.wait()

        u = act[...]
        for c in range(NC):
            give_part(i, 1, c, dot(u, wd[:, pl.ds(c * width, width)]))

    def mlp_sum(i):
        @pl.when(is_mid & (pp < last))
        def _():
            for c in range(NC):
                nxt[i, c] = (hmid[i, c].astype(F32) + total_of(i, 1, c)).astype(BF16)
                for copy in to_next(i, c):
                    copy.start()

        @pl.when(is_mid & (pp == last))
        def _():
            for c in range(NC):
                fin[i, c] = (hmid[i, c].astype(F32) + total_of(i, 1, c)).astype(BF16)
                fin_copy(i, c, 0, side, last).start()
                fin_copy(i, c, 1, tp, last - 2).start()
                fin_copy(i, c, 2, tp, last - 1).start()

        @pl.when(is_end & (pp == last))
        def _():
            for c in range(NC):
                fin_copy(i, c, 0, side, last).wait_recv()
                fin_copy(i, c, 1, tp, last - 2).start()
                fin_copy(i, c, 2, tp, last - 1).start()

    @pl.loop(0, nm)
    def _(i):
        first = i == 0
        attention(i, first)
        mid_sum(i, 0)
        attention_sum(i)
        mlp(i, first)
        mid_sum(i, 1)
        mlp_sum(i)

    @pl.loop(0, nm)
    def _(i):
        @pl.when(pp < last)
        def _():
            for c in range(NC):
                fin_copy(i, c, 0, side, last).wait_recv()

                @pl.when(pp == last - 2)
                def _():
                    fin_copy(i, c, 0, tp, 0).start()

        for c in range(NC):
            out_ref[i, :, pl.ds(c * width, width)] = fin[i, c]

    @pl.loop(0, nm)
    def _(i):
        for c in range(NC):
            for k in range(2):
                end_to_mid(i, k, c).wait_send()

            @pl.when(is_mid)
            def _():
                mid_to_end(i, c).wait_send()

            @pl.when(is_mid & (pp < last))
            def _():
                for copy in to_next(i, c):
                    copy.wait_send()

            @pl.when((is_mid & (pp == last)) | (pp == last - 2))
            def _():
                fin_copy(i, c, 0, side, last).wait_send()

            @pl.when(pp == last)
            def _():
                fin_copy(i, c, 1, side, last).wait_send()
                fin_copy(i, c, 2, side, last).wait_send()


def run_layers(hidden, positions, key_cache, value_cache, attn_norm, w_query, w_key, w_value, w_out, mlp_norm, w_gate, w_up, w_down):
    n_groups, n_batch, d_model = hidden.shape
    seq, head = key_cache.shape[-2:]
    nm = n_groups * n_batch // T
    ff = w_gate.shape[-1]
    width = d_model // NC
    angles = positions.astype(F32)[..., None] * rope_freqs(head)
    cosine, sine = jnp.cos(angles), jnp.sin(angles)
    cos_t = jnp.concatenate([cosine] * 4, axis=-1).reshape(nm, T, 128)
    sin_t = jnp.concatenate([-sine, sine, -sine, sine], axis=-1).reshape(nm, T, 128)
    pos_t = jnp.broadcast_to(positions.reshape(nm, T, 1), (nm, T, 128))
    flat = lambda cache: jnp.swapaxes(cache, -1, -2).reshape(nm, T * head, seq)
    any_spec = pl.BlockSpec(memory_space=pl.ANY)
    vmem_spec = pl.BlockSpec(memory_space=pltpu.VMEM)
    dma = pltpu.SemaphoreType.DMA
    scratch = [
        pltpu.VMEM((d_model, 512), BF16),
        pltpu.VMEM((128, d_model), BF16),
        pltpu.VMEM((512, d_model), BF16),
        pltpu.VMEM((d_model, 2 * ff), BF16),
        pltpu.VMEM((ff, d_model), BF16),
        pltpu.VMEM((nm, T * head, seq), BF16),
        pltpu.VMEM((nm, T * head, seq), BF16),
        pltpu.VMEM((nm, NC, T, width), BF16),
        pltpu.VMEM((nm, NC, T, width), BF16),
        pltpu.VMEM((T, d_model), BF16),
        pltpu.VMEM((T, 512), F32),
        pltpu.VMEM((T, 128), F32),
        pltpu.VMEM((T, 128), F32),
        pltpu.VMEM((T, 512), F32),
        pltpu.VMEM((T, ff), BF16),
        pltpu.VMEM((nm, NC, T, width), F32),
        pltpu.VMEM((nm, 2, NC, T, width), BF16),
        pltpu.VMEM((nm, 2, NC, T, width), BF16),
        pltpu.VMEM((nm, 2, NC, T, width), BF16),
        pltpu.VMEM((nm, NC, T, width), BF16),
        pltpu.VMEM((nm, NC, T, width), BF16),
        dma((5 + 2 * (ff // 128),)),
        dma((2, nm)),
        dma((nm, NC)),
        dma((nm, NC)),
        dma((nm, NC)),
        dma((nm, 2, NC)),
        dma((nm, 2, NC)),
        dma((nm, NC)),
        dma((nm, 2, NC)),
        dma((nm, NC)),
        dma((nm, NC, 2)),
        dma((nm, NC, 3)),
    ]
    out, kv = pl.pallas_call(
        functools.partial(layer_kernel, nm),
        out_shape=(jax.ShapeDtypeStruct((nm, T, d_model), BF16), jax.ShapeDtypeStruct((nm, T, 2 * head), BF16)),
        in_specs=[any_spec] + [vmem_spec] * 5 + [any_spec] * 9,
        out_specs=(vmem_spec, vmem_spec),
        scratch_shapes=scratch,
        compiler_params=pltpu.CompilerParams(collective_id=0, has_side_effects=True, vmem_limit_bytes=64000000),
        name="layers",
    )(
        hidden.reshape(nm, T, d_model), pos_t, cos_t, sin_t, attn_norm, mlp_norm,
        w_query[0], jnp.swapaxes(w_key[0], 0, 1), jnp.swapaxes(w_value[0], 0, 1), w_out[0], w_gate[0], w_up[0], w_down[0],
        flat(key_cache[0]), flat(value_cache[0]),
    )
    kv = kv.reshape(n_groups, n_batch, 2 * head)
    row_hit = (jnp.arange(seq) == positions[..., None])[None, :, :, None, :, None]
    key_out = jnp.where(row_hit, kv[None, :, :, None, None, :head], key_cache)
    value_out = jnp.where(row_hit, kv[None, :, :, None, None, head:], value_cache)
    return out.reshape(n_groups, n_batch, d_model), key_out, value_out


def solution(mesh):
    cache_spec = P("pp", "dp", None, "tp", None, None)
    col_spec = P("pp", None, "tp")
    row_spec = P("pp", "tp", None)
    gain_spec = P("pp", None)
    in_specs = (P("dp", None, None), P("dp", None), cache_spec, cache_spec, gain_spec, col_spec, col_spec, col_spec, row_spec, gain_spec, col_spec, col_spec, row_spec)
    out_specs = (P("dp", None, None), cache_spec, cache_spec)
    return jax.shard_map(run_layers, mesh=mesh, in_specs=in_specs, out_specs=out_specs, check_vma=False)
```
